256 devices in a mesh: dp: 32 (over y, z_hi, x), tensor: 8 (over z_lo, core).
Axes of the slice: x: 4, y: 4, z: 8 (z_hi: 2, z_lo: 4; z = z_hi * 4 + z_lo), core: 2. Of those that a mesh axis runs over, the one named last changes fastest.
Arguments:
- tokens: bfloat16 [1536, 6144], P('dp', 'tensor'), may hold values from -6 to 6
- out_grad: bfloat16 [1536, 6144], P('dp', 'tensor'), may hold values from -1.5 to 1.5
- expert_ids: int32 [1536, 2], P('dp'), may hold values from 0 to 3, all different within a row; in each aligned block of 48 rows (0 to 47, 48 to 95, ...) at most 32 rows name the same one
- gate_prob: bfloat16 [1536, 2], P('dp'), may hold values from 0.19921875 to 1
- gate_weight: bfloat16 [6144, 32768], P('tensor', 'dp'), may hold values from -0.078125 to 0.078125
- up_weight: bfloat16 [6144, 32768], P('tensor', 'dp'), may hold values from -0.078125 to 0.078125
- down_weight: bfloat16 [32768, 6144], P('dp', 'tensor'), may hold values from -0.0625 to 0.0625
Outputs:
- input_grad: bfloat16 [1536, 6144], P('dp', 'tensor')
- prob_grad: float32 [1536, 2], P('dp')
- gate_grad: bfloat16 [6144, 32768], P('tensor', 'dp')
- up_grad: bfloat16 [6144, 32768], P('tensor', 'dp')
- down_grad: bfloat16 [32768, 6144], P('dp', 'tensor')
The draws below stay inside these ranges and needn't reach their ends.
Inputs may be any that keep to these rules, and one draw needn't show every extreme that they name: `expert_ids`: the two ids of a token differ. Among the 48 tokens of one index of dp (aligned blocks of rows), no expert is named by more than 32 tokens, a bound that some block reaches.
All inputs are finite; a program needn't handle non-finite values.
Results may differ from the reference program's by a relative error of at most 0.0057.
Values may be sent and summed in bfloat16 or wider, within the bound.
No kernel may reach another device: no remote copies, remote signals or barrier semaphores. Data moves between devices by JAX's collectives and lax.ppermute only.
A program may use at most 128 MiB of HBM per device.

```python
import math
import jax
import jax.numpy as jnp
import numpy as np

D = 6144
HID = 8192
EXPERTS = 4
TOK_DP = 48
CAP = 32
TOKENS = 1536
N_DP = 32


def block_levels(stream_key, dims, cuts, low, largest):
    def one(dim, shards_of):
        heights = jax.random.uniform(jax.random.fold_in(jax.random.fold_in(stream_key, 6), dim), (shards_of,), jnp.float32, low / len(cuts), largest / len(cuts))
        return jnp.repeat(jnp.exp(heights), dims[dim] // shards_of).reshape((-1,) + (1,) * (len(dims) - dim - 1))

    factor_of = one(*cuts[0])
    for cut in cuts[1:]:
        factor_of = factor_of * one(*cut)
    return factor_of


def shared_out(rng, own, number, rows, amount, top, reach, lean):
    ranking = jax.random.permutation(rng, amount)
    heavy_load, usual = load_shares(amount, rows * top, reach, lean, True), load_shares(amount, rows * top, reach, lean, False)
    places = jnp.arange(amount)

    def named(sizes, turn):
        used = int((sizes > 0).sum())
        fixed = max(1, used // 4)
        passed = fixed + (places - fixed + turn * (used - fixed)) % max(1, amount - fixed)
        return jnp.zeros((amount,), jnp.int32).at[ranking[jnp.where(places < fixed, places, passed)]].set(jnp.asarray(sizes, jnp.int32))

    sizes = jnp.where(number % 4 == 0, named(heavy_load, number // 4), named(usual, number - number // 4 - 1))
    mixed = jax.random.permutation(jax.random.fold_in(own, 3), amount)
    giver, sink = mixed[0:amount // 2 * 2:2], mixed[1:amount // 2 * 2:2]
    slack = jnp.minimum(sizes[giver] - 1, reach - sizes[sink]) // 2
    slack = jnp.where((giver == ranking[0]) | (sink == ranking[0]) | (sizes[sink] == 0), 0, jnp.maximum(slack, 0))
    passed = jax.random.randint(jax.random.fold_in(own, 4), (amount // 2,), 0, 1 << 20) % (slack + 1)
    sizes = sizes.at[giver].add(-passed).at[sink].add(passed)
    items = jnp.searchsorted(jnp.cumsum(sizes), jnp.arange(rows * top), side="right").astype(jnp.int32)
    listing = items.reshape(top, rows).T
    listing = listing[jax.random.permutation(jax.random.fold_in(own, 1), rows)]
    turn = jax.random.randint(jax.random.fold_in(own, 2), (rows, 1), 0, top)
    return jnp.take_along_axis(listing, (jnp.arange(top)[None, :] + turn) % top, axis=1)


def load_shares(count, total, limit, slope, full):
    weights = [(1 << 20) // math.isqrt(grade ** slope) + 1 for grade in range(1, count + 1)]
    largest = limit if full else min(limit, max(-(-total // count), total * weights[0] // sum(weights)))
    least = 1 if total - largest >= count - 1 else 0
    counts, rest = [largest] + [least] * (count - 1), total - largest - least * (count - 1)
    while rest > 0:
        free = [i for i in range(1, count) if counts[i] < largest] or [i for i in range(1, count) if counts[i] < limit]
        whole, budget = sum([weights[i] for i in free]), rest
        for i in free:
            addition = min(limit - counts[i], max(1, budget * weights[i] // whole), rest)
            counts[i] = counts[i] + addition
            rest = rest - addition
    return np.array(counts)


def normal_values(stream_key, extent, width, reach, cuts=(), kind=jnp.bfloat16):
    result = width * jax.random.normal(stream_key, extent, jnp.float32)
    if cuts:
        result = result * block_levels(stream_key, extent, cuts, -0.22, 0.18)
    return jnp.clip(result, -reach, reach).astype(kind)


def setup_inputs(seed: int = 0) -> dict:
    key_of = jax.random.split(jax.random.key(seed), 8)
    tokens = normal_values(key_of[0], (TOKENS, D), 1.0, 6.0, ((0, 32), (1, 8)))
    out_grad = normal_values(key_of[1], (TOKENS, D), 0.25, 1.5, ((0, 32), (1, 8)))
    expert_ids_keys = jax.random.split(jax.random.fold_in(key_of[2], 1), TOKENS // TOK_DP)
    expert_ids_turns = jax.random.permutation(jax.random.fold_in(key_of[2], 3), TOKENS // TOK_DP)
    expert_ids = jax.vmap(lambda own, number: shared_out(jax.random.fold_in(key_of[2], 2), own, number, TOK_DP, EXPERTS, 2, CAP, 2))(expert_ids_keys, expert_ids_turns).reshape((TOKENS, 2))
    gate_prob = jnp.clip(0.19921875 + 0.80078125 * jax.random.uniform(key_of[3], (TOKENS, 2), jnp.float32) ** block_levels(key_of[3], (TOKENS, 2), ((0, 32),), -0.2, 0.2), 0.19921875, 1.0).astype(jnp.bfloat16)
    gate_weight = normal_values(key_of[4], (D, EXPERTS * HID), D ** -0.5, 0.078125, ((0, 8), (1, 32)))
    up_weight = normal_values(key_of[5], (D, EXPERTS * HID), D ** -0.5, 0.078125, ((0, 8), (1, 32)))
    down_weight = normal_values(key_of[6], (EXPERTS * HID, D), HID ** -0.5, 0.0625, ((0, 32), (1, 8)))
    return {"tokens": tokens, "out_grad": out_grad, "expert_ids": expert_ids, "gate_prob": gate_prob, "gate_weight": gate_weight, "up_weight": up_weight, "down_weight": down_weight}


def slot_positions(expert_ids):
    labels = expert_ids.reshape(N_DP, 2 * TOK_DP).astype(jnp.int32)
    onehot = (labels[:, :, None] == jnp.arange(EXPERTS, dtype=jnp.int32)[None, None, :]).astype(jnp.int32)
    before = (jnp.cumsum(onehot, axis=1) - onehot).astype(jnp.int32)
    places = jnp.sum(before * onehot, axis=2).astype(jnp.int32)
    return labels, places


def reference(tokens, out_grad, expert_ids, gate_prob, gate_weight, up_weight, down_weight):
    labels, places = slot_positions(expert_ids)
    block_ids = jnp.arange(N_DP, dtype=jnp.int32)[:, None]
    slot_ids = (block_ids * (2 * TOK_DP) + jnp.arange(2 * TOK_DP, dtype=jnp.int32)[None, :]).reshape(-1).astype(jnp.int32)
    padded_tokens = jnp.concatenate([jnp.repeat(tokens, 2, axis=0), jnp.zeros((1, D), jnp.bfloat16)], axis=0)
    padded_grads = jnp.concatenate([jnp.repeat(out_grad, 2, axis=0), jnp.zeros((1, D), jnp.bfloat16)], axis=0)
    padded_probs = jnp.concatenate([gate_prob.reshape(-1).astype(jnp.float32), jnp.zeros((1,), jnp.float32)], axis=0)
    slot_grad = jnp.zeros((2 * TOKENS, D), jnp.float32)
    prob_slots = jnp.zeros((2 * TOKENS,), jnp.float32)
    gate_parts = []
    up_parts = []
    down_parts = []
    for expert in range(EXPERTS):
        target = jnp.where(labels == expert, block_ids * CAP + places, N_DP * CAP).reshape(-1).astype(jnp.int32)
        picked = jnp.full((N_DP * CAP,), 2 * TOKENS, jnp.int32).at[target].set(slot_ids, mode="drop")
        rows_in = padded_tokens[picked]
        grads_in = padded_grads[picked]
        probs_in = padded_probs[picked]
        gate_cols = gate_weight[:, expert * HID:(expert + 1) * HID]
        up_cols = up_weight[:, expert * HID:(expert + 1) * HID]
        down_rows = down_weight[expert * HID:(expert + 1) * HID, :]
        pre_gate = jnp.dot(rows_in, gate_cols, preferred_element_type=jnp.float32)
        pre_up = jnp.dot(rows_in, up_cols, preferred_element_type=jnp.float32)
        sigmoid_gate = jax.nn.sigmoid(pre_gate)
        hidden = (pre_gate * sigmoid_gate * pre_up).astype(jnp.bfloat16)
        back_hidden = jnp.dot(grads_in, down_rows.T, preferred_element_type=jnp.float32)
        prob_term = jnp.sum(hidden.astype(jnp.float32) * back_hidden, axis=1)
        hidden_grad = probs_in[:, None] * back_hidden
        gate_pre = (hidden_grad * pre_up * sigmoid_gate * (1.0 + pre_gate * (1.0 - sigmoid_gate))).astype(jnp.bfloat16)
        up_pre = (hidden_grad * pre_gate * sigmoid_gate).astype(jnp.bfloat16)
        scaled = (probs_in[:, None] * grads_in.astype(jnp.float32)).astype(jnp.bfloat16)
        input_part = jnp.dot(gate_pre, gate_cols.T, preferred_element_type=jnp.float32) + jnp.dot(up_pre, up_cols.T, preferred_element_type=jnp.float32)
        gate_parts.append(jnp.dot(rows_in.T, gate_pre, preferred_element_type=jnp.float32).astype(jnp.bfloat16))
        up_parts.append(jnp.dot(rows_in.T, up_pre, preferred_element_type=jnp.float32).astype(jnp.bfloat16))
        down_parts.append(jnp.dot(hidden.T, scaled, preferred_element_type=jnp.float32).astype(jnp.bfloat16))
        slot_grad = slot_grad.at[picked].add(input_part, mode="drop")
        prob_slots = prob_slots.at[picked].add(prob_term, mode="drop")
    input_grad = jnp.sum(slot_grad.reshape(TOKENS, 2, D), axis=1).astype(jnp.bfloat16)
    prob_grad = prob_slots.reshape(TOKENS, 2)
    gate_grad = jnp.concatenate(gate_parts, axis=1)
    up_grad = jnp.concatenate(up_parts, axis=1)
    down_grad = jnp.concatenate(down_parts, axis=0)
    return (input_grad, prob_grad, gate_grad, up_grad, down_grad)
```

```python
import jax
import jax.numpy as jnp
from jax import lax
from jax.sharding import Mesh, PartitionSpec as P

EXPERTS = 4
CAP = 32
CHUNKS = 2
ROWS = CAP // CHUNKS
FINE = (("y", 4), ("zh", 2), ("x", 4), ("zl", 4), ("c", 2))

bf16, f32 = jnp.bfloat16, jnp.float32
precise = lax.Precision.HIGHEST


def ring(n, step):
    return [(i, (i + step) % n) for i in range(n)]


def dot(left, right, dims):
    return lax.dot_general(left, right, (dims, ((), ())), preferred_element_type=f32)


def slot_table(expert_ids, y):
    labels = jnp.bitwise_and(expert_ids.reshape(-1) - y, EXPERTS - 1)
    onehot = (labels[:, None] == jnp.arange(EXPERTS, dtype=jnp.int32)[None, :]).astype(jnp.int32)
    before = jnp.cumsum(onehot, axis=0) - onehot
    places = jnp.sum(before * onehot, axis=1)
    codes = labels * CAP + places
    return jnp.arange(EXPERTS * CAP, dtype=jnp.int32)[:, None] == codes[None, :]


def dispatch(block):
    got = [block[0]] + [lax.ppermute(block[j], "y", ring(4, j)) for j in range(1, 4)]
    mine = jnp.concatenate(got, axis=0)
    other = lax.ppermute(mine, "zh", ring(2, 1))
    b0 = jnp.concatenate([mine, other], axis=0)
    half = b0.shape[0] // 2
    b1 = lax.ppermute(b0, "x", ring(4, -1))
    b3 = lax.ppermute(b0, "x", ring(4, 1))
    b2 = jnp.concatenate(
        [lax.ppermute(b1[:half], "x", ring(4, -1)), lax.ppermute(b3[half:], "x", ring(4, 1))], axis=0
    )
    return [b0, b1, b2, b3]


def turned(blocks, shift):
    n = blocks[0].shape[0]
    both = jnp.concatenate(blocks + blocks[:3], axis=0)
    return lax.dynamic_slice_in_dim(both, shift * n, 4 * n, axis=0)


def line_sum(part):
    right = left = None
    for t in range(1, 4):
        r = part(4 - t) if right is None else part(4 - t) + right.astype(f32)
        l = part(t) if left is None else part(t) + left.astype(f32)
        right = lax.ppermute(r.astype(bf16), "zl", [(i, i + 1) for i in range(t)])
        left = lax.ppermute(l.astype(bf16), "zl", [(3 - i, 2 - i) for i in range(t)])
    return part(0) + right.astype(f32) + left.astype(f32)


def line_gather(own):
    right, left, rights, lefts = own, own, [], []
    for t in range(1, 4):
        right = lax.ppermute(right, "zl", [(i, i + 1) for i in range(t - 1, 3)])
        left = lax.ppermute(left, "zl", [(3 - i, 2 - i) for i in range(t - 1, 3)])
        rights.append(right)
        lefts.append(left)
    return [own] + [lefts[j - 1] + rights[3 - j] for j in range(1, 4)]


def body(tokens, out_grad, expert_ids, gate_prob, gate_weight, up_weight, down_weight):
    y, zl, c = lax.axis_index("y"), lax.axis_index("zl"), lax.axis_index("c")
    width = tokens.shape[1]
    hid = gate_weight.shape[1]
    half = hid // 2

    selector = slot_table(expert_ids, y)
    token_pick = jnp.any(selector.reshape(EXPERTS * CAP, -1, 2), axis=2).astype(bf16)
    slot_pick = selector.astype(bf16)
    both = jnp.concatenate([tokens, out_grad], axis=1)
    send_rows = dot(token_pick, both, ((1,), (0,))).astype(bf16)
    send_probs = dot(slot_pick, gate_prob.reshape(-1, 1), ((1,), (0,))).astype(bf16)
    send = jnp.concatenate([send_rows, jnp.broadcast_to(send_probs, (EXPERTS * CAP, 128))], axis=1)
    send = send.reshape(EXPERTS, CHUNKS, ROWS, 2 * width + 128)

    def swapped(weight, axis):
        own = lax.dynamic_slice_in_dim(weight, c * half, half, axis)
        other = lax.dynamic_slice_in_dim(weight, (1 - c) * half, half, axis)
        return jnp.concatenate([own, lax.ppermute(other, "c", ring(2, 1))], axis=1 - axis)

    wide_in = jnp.concatenate([swapped(gate_weight, 1), swapped(up_weight, 1)], axis=1)
    wide_out = swapped(down_weight, 0)

    rows, grads, probs_of, acts, prob_parts, back = [], [], [], [], [], []
    for k in range(CHUNKS):
        with jax.named_scope(f"arrive{k}"):
            blocks = dispatch(send[:, k])
            n = blocks[0].shape[0]
            all_in = turned(blocks, zl)
            mate = lax.ppermute(all_in[:, : 2 * width], "c", ring(2, 1))
            own_rows, own_grads = all_in[:, :width], all_in[:, width : 2 * width]
            probs = all_in[:, 2 * width : 2 * width + 1].astype(f32)
        with jax.named_scope(f"forward{k}"):
            wide_rows = jnp.concatenate([own_rows, mate[:, :width]], axis=1)
            wide_grads = jnp.concatenate([own_grads, mate[:, width:]], axis=1)
            pre = dot(wide_rows, wide_in, ((1,), (0,)))
            bh = dot(wide_grads, wide_out, ((1,), (1,)))
        with jax.named_scope(f"sum{k}"):
            total = line_sum(
                lambda j: jnp.concatenate([pre[j * n : j * n + n], bh[j * n : j * n + n]], axis=1)
            )
        with jax.named_scope(f"middle{k}"):
            pre_gate, pre_up, back_hidden = total[:, :half], total[:, half:hid], total[:, hid:]
            sig = jax.nn.sigmoid(pre_gate)
            hidden = (pre_gate * sig * pre_up).astype(bf16)
            hidden_grad = probs[:n] * back_hidden
            gate_pre = (hidden_grad * pre_up * sig * (1.0 + pre_gate * (1.0 - sig))).astype(bf16)
            up_pre = (hidden_grad * pre_gate * sig).astype(bf16)
            prob_parts.append(jnp.sum(hidden.astype(f32) * back_hidden, axis=1))
            share = jnp.concatenate([hidden, gate_pre, up_pre], axis=1)
        with jax.named_scope(f"gather{k}"):
            act = jnp.concatenate(line_gather(share), axis=0)
            act_mate = lax.ppermute(act, "c", ring(2, 1))
            low = jnp.where(c == 0, act, act_mate)
            high = jnp.where(c == 0, act_mate, act)
            act = [
                jnp.concatenate([low[:, i * half : i * half + half], high[:, i * half : i * half + half]], axis=1)
                for i in range(3)
            ]
        with jax.named_scope(f"input{k}"):
            part = dot(act[1], gate_weight, ((1,), (1,))) + dot(act[2], up_weight, ((1,), (1,)))
        with jax.named_scope(f"return{k}"):

            def piece(j):
                return lax.dynamic_slice_in_dim(part, jnp.bitwise_and(j - zl, 3) * n, n, axis=0)

            summed = piece(0)
            for j in range(1, 4):
                summed = summed + lax.ppermute(piece(j).astype(bf16), "x", ring(4, j)).astype(f32)
            m = n // 2
            summed = summed[:m] + lax.ppermute(summed[m:].astype(bf16), "zh", ring(2, 1)).astype(f32)
            summed = summed.reshape(EXPERTS, ROWS, width)
            back.append(
                jnp.stack([summed[0]] + [lax.ppermute(summed[j], "y", ring(4, -j)) for j in range(1, 4)])
            )
        rows.append(own_rows)
        grads.append(own_grads)
        probs_of.append(probs)
        acts.append(act)

    with jax.named_scope("prob"):
        v = jnp.stack(prob_parts)
        v = v + lax.ppermute(v, "c", ring(2, 1))
        v = lax.ppermute(v, ("x", "zl"), [(4 * a + b, 4 * ((a + b) % 4) + b) for a in range(4) for b in range(4)])
        v = v + sum(lax.ppermute(v, "zl", ring(4, j)) for j in range(1, 4))
        m = v.shape[1] // 2
        v = v[:, :m] + lax.ppermute(v[:, m:], "zh", ring(2, 1))
        v = v.reshape(CHUNKS, EXPERTS, ROWS)
        v = jnp.stack([v[:, 0]] + [lax.ppermute(v[:, j], "y", ring(4, -j)) for j in range(1, 4)])
        summed_probs = v.reshape(EXPERTS * CAP)

    with jax.named_scope("weights"):
        all_rows, all_grads = jnp.concatenate(rows, axis=0), jnp.concatenate(grads, axis=0)
        all_probs = jnp.concatenate(probs_of, axis=0)
        hidden, gate_pre, up_pre = (jnp.concatenate([a[i] for a in acts], axis=0) for i in range(3))
        scaled = (all_probs * all_grads.astype(f32)).astype(bf16)
        gate_grad = dot(all_rows, gate_pre, ((0,), (0,))).astype(bf16)
        up_grad = dot(all_rows, up_pre, ((0,), (0,))).astype(bf16)
        down_grad = dot(hidden, scaled, ((0,), (0,))).astype(bf16)

    summed_rows = jnp.concatenate(back, axis=1).reshape(EXPERTS * CAP, width)
    input_grad = lax.dot_general(
        token_pick.astype(f32),
        summed_rows,
        (((0,), (0,)), ((), ())),
        precision=precise,
        preferred_element_type=f32,
    ).astype(bf16)
    prob_grad = lax.dot_general(
        slot_pick.astype(f32),
        summed_probs,
        (((0,), (0,)), ((), ())),
        precision=precise,
        preferred_element_type=f32,
    ).reshape(-1, 2)
    return (input_grad, prob_grad, gate_grad, up_grad, down_grad)


def solution(mesh):
    names, sizes = zip(*FINE)
    fine = Mesh(mesh.devices.reshape(sizes), names)
    dp, tensor = ("y", "zh", "x"), ("zl", "c")
    return jax.shard_map(
        body,
        mesh=fine,
        in_specs=(
            P(dp, tensor),
            P(dp, tensor),
            P(dp, None),
            P(dp, None),
            P(tensor, dp),
            P(tensor, dp),
            P(dp, tensor),
        ),
        out_specs=(
            P(dp, tensor),
            P(dp, None),
            P(tensor, dp),
            P(tensor, dp),
            P(dp, tensor),
        ),
        check_vma=False,
    )
```

```python
import jax
import jax.numpy as jnp
from jax import lax
from jax.experimental import pallas as pl
from jax.experimental.pallas import tpu as pltpu
from jax.sharding import Mesh, PartitionSpec as P


EXPERTS = 4
CAP = 32
FINE = (("y", 4), ("zh", 2), ("x", 4), ("zl", 4), ("c", 2))

bf16, f32 = jnp.bfloat16, jnp.float32
precise = lax.Precision.HIGHEST


def ring(n, step):
    return [(i, (i + step) % n) for i in range(n)]


def moved(value, axis, pairs):
    return lax.ppermute(value, axis, pairs)


def dot(left, right, dims):
    return lax.dot_general(left, right, (dims, ((), ())), preferred_element_type=f32)


def slot_table(expert_ids, y):
    labels = jnp.bitwise_and(expert_ids.reshape(-1) - y, EXPERTS - 1)
    onehot = (labels[:, None] == jnp.arange(EXPERTS, dtype=jnp.int32)[None, :]).astype(jnp.int32)
    before = jnp.cumsum(onehot, axis=0) - onehot
    places = jnp.sum(before * onehot, axis=1)
    codes = labels * CAP + places
    return jnp.arange(EXPERTS * CAP, dtype=jnp.int32)[:, None] == codes[None, :]


def dispatch(block):
    got = [block[0]] + [moved(block[j], "y", ring(4, j)) for j in range(1, 4)]
    mine = jnp.concatenate(got, axis=0)
    h = mine.shape[0]
    b0 = jnp.concatenate([mine, moved(mine, "zh", ring(2, 1))], axis=0)
    b1 = moved(b0, "x", ring(4, -1))
    b3 = moved(b0, "x", ring(4, 1))
    b2a = moved(b1[:h], "x", ring(4, -1))
    b2b = moved(b3[h:], "x", ring(4, 1))
    return jnp.concatenate([b0, b1, b2a, b2b, b3], axis=0)


def ring_sum(part):
    right = left = None
    for t in range(1, 4):
        r = part(4 - t, 0) if right is None else part(4 - t, 0) + right.astype(f32)
        l = part(t, 1) if left is None else part(t, 1) + left.astype(f32)
        right = moved(r.astype(bf16), "zl", ring(4, 1))
        left = moved(l.astype(bf16), "zl", ring(4, -1))
        right, left = lax.optimization_barrier((right, left))
    return jnp.concatenate([part(0, 0) + right.astype(f32), part(0, 1) + left.astype(f32)], axis=0)


def laid_out(zl, own, rights, lefts):
    n, width = own.shape
    h = n // 2

    def copy(at, own, r1, r2, r3, l1, l2, l3, out):
        i = at[0]

        def put(first, value):
            out[pl.ds(pl.multiple_of(first, h), h), :] = value

        put(i * n, own[:h, :])
        put(i * n + h, own[h:, :])
        for t, (r, l) in enumerate(((r1, l1), (r2, l2), (r3, l3)), start=1):
            put(((i + 4 - t) & 3) * n, r[...])
            put(((i + t) & 3) * n + h, l[...])

    whole = pl.BlockSpec(memory_space=pltpu.VMEM)
    return pl.pallas_call(
        copy,
        out_shape=jax.ShapeDtypeStruct((4 * n, width), own.dtype),
        in_specs=[pl.BlockSpec(memory_space=pltpu.SMEM)] + [whole] * 7,
        out_specs=whole,
    )(zl.reshape(1), own, *rights, *lefts)


def ring_gather(own, zl):
    h = own.shape[0] // 2
    rights, lefts = [own[:h]], [own[h:]]
    for _ in range(1, 4):
        rights.append(moved(rights[-1], "zl", ring(4, 1)))
        lefts.append(moved(lefts[-1], "zl", ring(4, -1)))
    return laid_out(zl, own, rights[1:], lefts[1:])


def body(tokens, out_grad, expert_ids, gate_prob, gate_weight, up_weight, down_weight):
    y, zl, c = lax.axis_index("y"), lax.axis_index("zl"), lax.axis_index("c")
    width = tokens.shape[1]
    hid = gate_weight.shape[1]
    half = hid // 2

    selector = slot_table(expert_ids, y)
    token_pick = jnp.any(selector.reshape(EXPERTS * CAP, -1, 2), axis=2).astype(bf16)
    slot_pick = selector.astype(bf16)
    send_rows = dot(token_pick, tokens, ((1,), (0,))).astype(bf16)
    send_grads = dot(token_pick, out_grad, ((1,), (0,))).astype(bf16)
    send_probs = dot(slot_pick, gate_prob.reshape(-1, 1), ((1,), (0,))).astype(bf16)
    send_grads = jnp.concatenate([send_grads, jnp.broadcast_to(send_probs, (EXPERTS * CAP, 128))], axis=1)

    def halves(weight, axis):
        return lax.optimization_barrier(
            [lax.dynamic_slice_in_dim(weight, s * half, half, axis) for s in (c, 1 - c)]
        )

    sides = [halves(gate_weight, 1), halves(up_weight, 1)]
    in_own, in_other = (jnp.concatenate([sides[0][s], sides[1][s]], axis=1) for s in range(2))
    out_own, out_other = halves(down_weight, 0)
    in_mate = moved(in_other, "c", ring(2, 1))
    out_mate = moved(out_other, "c", ring(2, 1))

    rows = dispatch(send_rows.reshape(EXPERTS, CAP, width))
    grads = dispatch(send_grads.reshape(EXPERTS, CAP, width + 128))
    n = rows.shape[0] // 4
    rows_mate = moved(rows, "c", ring(2, 1))
    grads_mate = moved(grads, "c", ring(2, 1))
    probs = grads[:, width:]
    own_grads = grads[:, :width]

    pre = dot(rows, in_own, ((1,), (0,))) + dot(rows_mate, in_mate, ((1,), (0,)))
    bh = dot(own_grads, out_own, ((1,), (1,))) + dot(grads_mate[:, :width], out_mate, ((1,), (1,)))

    def part_of(value):
        def part(j, s):
            at = jnp.bitwise_and(zl + j, 3) * n + s * (n // 2)
            return lax.dynamic_slice_in_dim(value, at, n // 2, axis=0)

        return part

    total = ring_sum(part_of(pre))
    back_hidden = ring_sum(part_of(bh))
    pre_gate, pre_up = total[:, :half], total[:, half:]
    sig = jax.nn.sigmoid(pre_gate)
    hidden = (pre_gate * sig * pre_up).astype(bf16)
    own_probs = lax.dynamic_slice_in_dim(probs, zl * n, n, axis=0)[:, :1].astype(f32)
    hidden_grad = own_probs * back_hidden
    gate_pre = (hidden_grad * pre_up * sig * (1.0 + pre_gate * (1.0 - sig))).astype(bf16)
    up_pre = (hidden_grad * pre_gate * sig).astype(bf16)
    prob_part = jnp.sum(hidden.astype(f32) * back_hidden, axis=1)

    act = ring_gather(jnp.concatenate([gate_pre, up_pre], axis=1), zl)
    act_mate = moved(act, "c", ring(2, 1))
    hid_own = ring_gather(hidden, zl)
    hid_mate = moved(hid_own, "c", ring(2, 1))

    back_in = dot(act, in_own, ((1,), (1,))) + dot(act_mate, in_other, ((1,), (1,)))
    h = n // 2
    far = back_in[2 * n : 3 * n].astype(bf16)
    from_left = moved(far[:h], "x", ring(4, 1)).astype(f32)
    from_right = moved(far[h:], "x", ring(4, -1)).astype(f32)
    one = jnp.concatenate([back_in[n : n + h] + from_left, back_in[n + h : 2 * n]], axis=0)
    three = jnp.concatenate([back_in[3 * n : 3 * n + h], back_in[3 * n + h :] + from_right], axis=0)
    summed = back_in[:n] + moved(one.astype(bf16), "x", ring(4, 1)).astype(f32)
    summed = summed + moved(three.astype(bf16), "x", ring(4, -1)).astype(f32)
    summed = summed[:h] + moved(summed[h:].astype(bf16), "zh", ring(2, 1)).astype(f32)
    summed = summed.reshape(EXPERTS, CAP, width)
    summed_rows = jnp.concatenate(
        [summed[0]] + [moved(summed[j], "y", ring(4, -j)) for j in range(1, 4)], axis=0
    )

    v = prob_part.reshape(2, n // 2)
    v = v + moved(v, "c", ring(2, 1))
    v = moved(v, ("x", "zl"), [(4 * a + b, 4 * ((a + b) % 4) + b) for a in range(4) for b in range(4)])
    v = v + sum(moved(v, "zl", ring(4, j)) for j in range(1, 4))
    v = v[0] + moved(v[1], "zh", ring(2, 1))
    v = v.reshape(EXPERTS, CAP)
    summed_probs = jnp.concatenate([v[0]] + [moved(v[j], "y", ring(4, -j)) for j in range(1, 4)])

    scaled = (probs[:, :1].astype(f32) * own_grads.astype(f32)).astype(bf16)

    def canonical(own, mate):
        return [jnp.where(c == 0, own, mate), jnp.where(c == 0, mate, own)]

    pair = canonical(act, act_mate)
    gate_all = jnp.concatenate([v[:, :half] for v in pair], axis=1)
    up_all = jnp.concatenate([v[:, half:] for v in pair], axis=1)
    hidden_all = jnp.concatenate(canonical(hid_own, hid_mate), axis=1)
    gate_grad = dot(rows, gate_all, ((0,), (0,))).astype(bf16)
    up_grad = dot(rows, up_all, ((0,), (0,))).astype(bf16)
    down_grad = dot(hidden_all, scaled, ((0,), (0,))).astype(bf16)

    input_grad = lax.dot_general(
        token_pick.astype(f32),
        summed_rows,
        (((0,), (0,)), ((), ())),
        precision=precise,
        preferred_element_type=f32,
    ).astype(bf16)
    prob_grad = lax.dot_general(
        slot_pick.astype(f32),
        summed_probs,
        (((0,), (0,)), ((), ())),
        precision=precise,
        preferred_element_type=f32,
    ).reshape(-1, 2)
    return (input_grad, prob_grad, gate_grad, up_grad, down_grad)


def solution(mesh):
    names, sizes = zip(*FINE)
    fine = Mesh(mesh.devices.reshape(sizes), names)
    dp, tensor = ("y", "zh", "x"), ("zl", "c")
    return jax.shard_map(
        body,
        mesh=fine,
        in_specs=(
            P(dp, tensor),
            P(dp, tensor),
            P(dp, None),
            P(dp, None),
            P(tensor, dp),
            P(tensor, dp),
            P(dp, tensor),
        ),
        out_specs=(
            P(dp, tensor),
            P(dp, None),
            P(tensor, dp),
            P(tensor, dp),
            P(dp, tensor),
        ),
        check_vma=False,
    )
```

```python
import jax
import jax.numpy as jnp
from jax import lax
from jax.experimental import pallas as pl
from jax.experimental.pallas import tpu as pltpu
from jax.sharding import Mesh, PartitionSpec as P


EXPERTS = 4
CAP = 32
FINE = (("y", 4), ("zh", 2), ("x", 4), ("zl", 4), ("c", 2))

bf16, f32 = jnp.bfloat16, jnp.float32
precise = lax.Precision.HIGHEST


def ring(n, step):
    return [(i, (i + step) % n) for i in range(n)]


def moved(value, axis, pairs):
    return lax.ppermute(value, axis, pairs)


def dot(left, right, dims):
    return lax.dot_general(left, right, (dims, ((), ())), preferred_element_type=f32)


def slot_table(expert_ids, y):
    labels = jnp.bitwise_and(expert_ids.reshape(-1) - y, EXPERTS - 1)
    onehot = (labels[:, None] == jnp.arange(EXPERTS, dtype=jnp.int32)[None, :]).astype(jnp.int32)
    before = jnp.cumsum(onehot, axis=0) - onehot
    places = jnp.sum(before * onehot, axis=1)
    codes = labels * CAP + places
    return jnp.arange(EXPERTS * CAP, dtype=jnp.int32)[:, None] == codes[None, :]


def dispatch(block):
    got = [block[0]] + [moved(block[j], "y", ring(4, j)) for j in range(1, 4)]
    mine = jnp.concatenate(got, axis=0)
    h = mine.shape[0]
    b0 = jnp.concatenate([mine, moved(mine, "zh", ring(2, 1))], axis=0)
    b1 = moved(b0, "x", ring(4, -1))
    b3 = moved(b0, "x", ring(4, 1))
    b2a = moved(b1[:h], "x", ring(4, -1))
    b2b = moved(b3[h:], "x", ring(4, 1))
    return jnp.concatenate([b0, b1, b2a, b2b, b3], axis=0)


def ring_sum(part):
    right = left = None
    for t in range(1, 4):
        r = part(4 - t, 0) if right is None else part(4 - t, 0) + right.astype(f32)
        l = part(t, 1) if left is None else part(t, 1) + left.astype(f32)
        right = moved(r.astype(bf16), "zl", ring(4, 1))
        left = moved(l.astype(bf16), "zl", ring(4, -1))
        right, left = lax.optimization_barrier((right, left))
    return jnp.concatenate([part(0, 0) + right.astype(f32), part(0, 1) + left.astype(f32)], axis=0)


def laid_out(zl, own, rights, lefts):
    n, width = own.shape
    h = n // 2

    def copy(at, own, r1, r2, r3, l1, l2, l3, out):
        i = at[0]

        def put(first, value):
            out[pl.ds(pl.multiple_of(first, h), h), :] = value

        put(i * n, own[:h, :])
        put(i * n + h, own[h:, :])
        for t, (r, l) in enumerate(((r1, l1), (r2, l2), (r3, l3)), start=1):
            put(((i + 4 - t) & 3) * n, r[...])
            put(((i + t) & 3) * n + h, l[...])

    whole = pl.BlockSpec(memory_space=pltpu.VMEM)
    return pl.pallas_call(
        copy,
        out_shape=jax.ShapeDtypeStruct((4 * n, width), own.dtype),
        in_specs=[pl.BlockSpec(memory_space=pltpu.SMEM)] + [whole] * 7,
        out_specs=whole,
    )(zl.reshape(1), own, *rights, *lefts)


def ring_gather(own, zl):
    h = own.shape[0] // 2
    rights, lefts = [own[:h]], [own[h:]]
    for _ in range(1, 4):
        rights.append(moved(rights[-1], "zl", ring(4, 1)))
        lefts.append(moved(lefts[-1], "zl", ring(4, -1)))
    return laid_out(zl, own, rights[1:], lefts[1:])


def body(tokens, out_grad, expert_ids, gate_prob, gate_weight, up_weight, down_weight):
    y, zl, c = lax.axis_index("y"), lax.axis_index("zl"), lax.axis_index("c")
    width = tokens.shape[1]
    hid = gate_weight.shape[1]
    half = hid // 2

    selector = slot_table(expert_ids, y)
    token_pick = jnp.any(selector.reshape(EXPERTS * CAP, -1, 2), axis=2).astype(bf16)
    slot_pick = selector.astype(bf16)
    send_rows = dot(token_pick, tokens, ((1,), (0,))).astype(bf16)
    send_grads = dot(token_pick, out_grad, ((1,), (0,))).astype(bf16)
    send_probs = dot(slot_pick, gate_prob.reshape(-1, 1), ((1,), (0,))).astype(bf16)
    send_grads = jnp.concatenate([send_grads, jnp.broadcast_to(send_probs, (EXPERTS * CAP, 128))], axis=1)

    def halves(weight, axis):
        return lax.optimization_barrier(
            [lax.dynamic_slice_in_dim(weight, s * half, half, axis) for s in (c, 1 - c)]
        )

    sides = [halves(gate_weight, 1), halves(up_weight, 1)]
    in_own, in_other = (jnp.concatenate([sides[0][s], sides[1][s]], axis=1) for s in range(2))
    out_own, out_other = halves(down_weight, 0)
    in_mate = moved(in_other, "c", ring(2, 1))
    out_mate = moved(out_other, "c", ring(2, 1))

    rows = dispatch(send_rows.reshape(EXPERTS, CAP, width))
    grads = dispatch(send_grads.reshape(EXPERTS, CAP, width + 128))
    n = rows.shape[0] // 4
    rows_mate = moved(rows, "c", ring(2, 1))
    grads_mate = moved(grads, "c", ring(2, 1))
    probs = grads[:, width:]
    own_grads = grads[:, :width]

    pre = dot(rows_mate, in_mate, ((1,), (0,)))
    pre = pre + dot(rows, in_own, ((1,), (0,)))
    bh = dot(grads_mate[:, :width], out_mate, ((1,), (1,)))
    bh = bh + dot(own_grads, out_own, ((1,), (1,)))

    def part_of(value):
        def part(j, s):
            at = jnp.bitwise_and(zl + j, 3) * n + s * (n // 2)
            return lax.dynamic_slice_in_dim(value, at, n // 2, axis=0)

        return part

    total = ring_sum(part_of(pre))
    back_hidden = ring_sum(part_of(bh))
    pre_gate, pre_up = total[:, :half], total[:, half:]
    sig = jax.nn.sigmoid(pre_gate)
    hidden = (pre_gate * sig * pre_up).astype(bf16)
    own_probs = lax.dynamic_slice_in_dim(probs, zl * n, n, axis=0)[:, :1].astype(f32)
    hidden_grad = own_probs * back_hidden
    gate_pre = (hidden_grad * pre_up * sig * (1.0 + pre_gate * (1.0 - sig))).astype(bf16)
    up_pre = (hidden_grad * pre_gate * sig).astype(bf16)
    prob_part = jnp.sum(hidden.astype(f32) * back_hidden, axis=1)

    act = ring_gather(jnp.concatenate([gate_pre, up_pre], axis=1), zl)
    act_mate = moved(act, "c", ring(2, 1))
    hid_own = ring_gather(hidden, zl)
    hid_mate = moved(hid_own, "c", ring(2, 1))

    back_in = dot(act, in_own, ((1,), (1,)))
    back_in = back_in + dot(act_mate, in_other, ((1,), (1,)))
    h = n // 2
    far = back_in[2 * n : 3 * n].astype(bf16)
    from_left = moved(far[:h], "x", ring(4, 1)).astype(f32)
    from_right = moved(far[h:], "x", ring(4, -1)).astype(f32)
    one = jnp.concatenate([back_in[n : n + h] + from_left, back_in[n + h : 2 * n]], axis=0)
    three = jnp.concatenate([back_in[3 * n : 3 * n + h], back_in[3 * n + h :] + from_right], axis=0)
    summed = back_in[:n] + moved(one.astype(bf16), "x", ring(4, 1)).astype(f32)
    summed = summed + moved(three.astype(bf16), "x", ring(4, -1)).astype(f32)
    summed = summed[:h] + moved(summed[h:].astype(bf16), "zh", ring(2, 1)).astype(f32)
    summed = summed.reshape(EXPERTS, CAP, width)
    summed_rows = jnp.concatenate([summed[0]] + [moved(summed[j], "y", ring(4, -j)) for j in range(1, 4)], axis=0)

    v = prob_part.reshape(2, n // 2)
    v = v + moved(v, "c", ring(2, 1))
    v = moved(v, ("x", "zl"), [(4 * a + b, 4 * ((a + b) % 4) + b) for a in range(4) for b in range(4)])
    v = v + sum(moved(v, "zl", ring(4, j)) for j in range(1, 4))
    v = v[0] + moved(v[1], "zh", ring(2, 1))
    v = v.reshape(EXPERTS, CAP)
    summed_probs = jnp.concatenate([v[0]] + [moved(v[j], "y", ring(4, -j)) for j in range(1, 4)])

    scaled = (probs[:, :1].astype(f32) * own_grads.astype(f32)).astype(bf16)

    def canonical(own, mate):
        return [jnp.where(c == 0, own, mate), jnp.where(c == 0, mate, own)]

    pair = canonical(act, act_mate)
    gate_all = jnp.concatenate([v[:, :half] for v in pair], axis=1)
    up_all = jnp.concatenate([v[:, half:] for v in pair], axis=1)
    hidden_all = jnp.concatenate(canonical(hid_own, hid_mate), axis=1)
    gate_grad = dot(rows, gate_all, ((0,), (0,))).astype(bf16)
    up_grad = dot(rows, up_all, ((0,), (0,))).astype(bf16)
    down_grad = dot(hidden_all, scaled, ((0,), (0,))).astype(bf16)

    input_grad = lax.dot_general(
        token_pick.astype(f32),
        summed_rows,
        (((0,), (0,)), ((), ())),
        precision=precise,
        preferred_element_type=f32,
    ).astype(bf16)
    prob_grad = lax.dot_general(
        slot_pick.astype(f32),
        summed_probs,
        (((0,), (0,)), ((), ())),
        precision=precise,
        preferred_element_type=f32,
    ).reshape(-1, 2)
    return (input_grad, prob_grad, gate_grad, up_grad, down_grad)


def solution(mesh):
    names, sizes = zip(*FINE)
    fine = Mesh(mesh.devices.reshape(sizes), names)
    dp, tensor = ("y", "zh", "x"), ("zl", "c")
    return jax.shard_map(
        body,
        mesh=fine,
        in_specs=(
            P(dp, tensor),
            P(dp, tensor),
            P(dp, None),
            P(dp, None),
            P(tensor, dp),
            P(tensor, dp),
            P(dp, tensor),
        ),
        out_specs=(
            P(dp, tensor),
            P(dp, None),
            P(tensor, dp),
            P(tensor, dp),
            P(dp, tensor),
        ),
        check_vma=False,
    )
```

```python
import jax
import jax.numpy as jnp
from jax import lax
from jax.experimental import pallas as pl
from jax.experimental.pallas import tpu as pltpu
from jax.sharding import Mesh, PartitionSpec as P


EXPERTS = 4
CAP = 32
FINE = (("y", 4), ("zh", 2), ("x", 4), ("zl", 4), ("c", 2))

bf16, f32 = jnp.bfloat16, jnp.float32
precise = lax.Precision.HIGHEST


def ring(n, step):
    return [(i, (i + step) % n) for i in range(n)]


def moved(value, axis, pairs):
    return lax.ppermute(value, axis, pairs)


def dot(left, right, dims):
    return lax.dot_general(left, right, (dims, ((), ())), preferred_element_type=f32)


def slot_table(expert_ids, y):
    labels = jnp.bitwise_and(expert_ids.reshape(-1) - y, EXPERTS - 1)
    onehot = (labels[:, None] == jnp.arange(EXPERTS, dtype=jnp.int32)[None, :]).astype(jnp.int32)
    before = jnp.cumsum(onehot, axis=0) - onehot
    places = jnp.sum(before * onehot, axis=1)
    codes = labels * CAP + places
    return jnp.arange(EXPERTS * CAP, dtype=jnp.int32)[:, None] == codes[None, :]


def dispatch(block):
    got = [block[0]] + [moved(block[j], "y", ring(4, j)) for j in range(1, 4)]
    mine = jnp.concatenate(got, axis=0)
    h = mine.shape[0]
    b0 = jnp.concatenate([mine, moved(mine, "zh", ring(2, 1))], axis=0)
    b1 = moved(b0, "x", ring(4, -1))
    b3 = moved(b0, "x", ring(4, 1))
    b2a = moved(b1[:h], "x", ring(4, -1))
    b2b = moved(b3[h:], "x", ring(4, 1))
    return jnp.concatenate([b0, b1, b2a, b2b, b3], axis=0)


def ring_sum(part):
    right = left = None
    for t in range(1, 4):
        r = part(4 - t, 0) if right is None else part(4 - t, 0) + right.astype(f32)
        l = part(t, 1) if left is None else part(t, 1) + left.astype(f32)
        right = moved(r.astype(bf16), "zl", ring(4, 1))
        left = moved(l.astype(bf16), "zl", ring(4, -1))
        right, left = lax.optimization_barrier((right, left))
    return jnp.concatenate([part(0, 0) + right.astype(f32), part(0, 1) + left.astype(f32)], axis=0)


def laid_out(zl, owns, rings):
    n, width = owns[0].shape
    h = n // 2

    def copy(at, *refs):
        out, i = refs[-1], at[0]
        for k in range(len(owns)):
            own, r1, r2, r3, l1, l2, l3 = refs[7 * k : 7 * k + 7]

            def put(first, value):
                out[pl.ds(pl.multiple_of(first, h), h), k * width : (k + 1) * width] = value

            put(i * n, own[:h, :])
            put(i * n + h, own[h:, :])
            for t, (r, l) in enumerate(((r1, l1), (r2, l2), (r3, l3)), start=1):
                put(((i + 4 - t) & 3) * n, r[...])
                put(((i + t) & 3) * n + h, l[...])

    whole = pl.BlockSpec(memory_space=pltpu.VMEM)
    pieces = sum([[own] + rights + lefts for own, (rights, lefts) in zip(owns, rings)], [])
    return pl.pallas_call(
        copy,
        out_shape=jax.ShapeDtypeStruct((4 * n, width * len(owns)), owns[0].dtype),
        in_specs=[pl.BlockSpec(memory_space=pltpu.SMEM)] + [whole] * len(pieces),
        out_specs=whole,
    )(zl.reshape(1), *pieces)


def ring_gather(own):
    h = own.shape[0] // 2
    rights, lefts = [own[:h]], [own[h:]]
    for _ in range(1, 4):
        rights.append(moved(rights[-1], "zl", ring(4, 1)))
        lefts.append(moved(lefts[-1], "zl", ring(4, -1)))
    return rights[1:], lefts[1:]


def body(tokens, out_grad, expert_ids, gate_prob, gate_weight, up_weight, down_weight):
    y, zl, c = lax.axis_index("y"), lax.axis_index("zl"), lax.axis_index("c")
    width = tokens.shape[1]
    hid = gate_weight.shape[1]
    half = hid // 2

    selector = slot_table(expert_ids, y)
    token_pick = jnp.any(selector.reshape(EXPERTS * CAP, -1, 2), axis=2).astype(bf16)
    slot_pick = selector.astype(bf16)
    send_rows = dot(token_pick, tokens, ((1,), (0,))).astype(bf16)
    send_grads = dot(token_pick, out_grad, ((1,), (0,))).astype(bf16)
    send_probs = dot(slot_pick, gate_prob.reshape(-1, 1), ((1,), (0,))).astype(bf16)
    send_grads = jnp.concatenate([send_grads, jnp.broadcast_to(send_probs, (EXPERTS * CAP, 128))], axis=1)

    def halves(weight, axis):
        return lax.optimization_barrier(
            [lax.dynamic_slice_in_dim(weight, s * half, half, axis) for s in (c, 1 - c)]
        )

    sides = [halves(gate_weight, 1), halves(up_weight, 1)]
    in_own, in_other = (jnp.concatenate([sides[0][s], sides[1][s]], axis=1) for s in range(2))
    out_own, out_other = halves(down_weight, 0)
    gate_mate = moved(sides[0][1], "c", ring(2, 1))
    up_mate = moved(sides[1][1], "c", ring(2, 1))
    out_mate = moved(out_other, "c", ring(2, 1))

    rows = dispatch(send_rows.reshape(EXPERTS, CAP, width))
    grads = dispatch(send_grads.reshape(EXPERTS, CAP, width + 128))
    n = rows.shape[0] // 4
    rows_mate = moved(rows, "c", ring(2, 1))
    grads_mate = moved(grads, "c", ring(2, 1))
    probs = grads[:, width:]
    own_grads = grads[:, :width]

    gate_sum = dot(rows_mate, gate_mate, ((1,), (0,)))
    gate_sum = gate_sum + dot(rows, sides[0][0], ((1,), (0,)))
    up_sum = dot(rows_mate, up_mate, ((1,), (0,)))
    up_sum = up_sum + dot(rows, sides[1][0], ((1,), (0,)))
    bh = dot(grads_mate[:, :width], out_mate, ((1,), (1,)))
    bh = bh + dot(own_grads, out_own, ((1,), (1,)))

    def part_of(value):
        def part(j, s):
            at = jnp.bitwise_and(zl + j, 3) * n + s * (n // 2)
            return lax.dynamic_slice_in_dim(value, at, n // 2, axis=0)

        return part

    pre_gate = ring_sum(part_of(gate_sum))
    pre_up = ring_sum(part_of(up_sum))
    back_hidden = ring_sum(part_of(bh))
    sig = jax.nn.sigmoid(pre_gate)
    hidden = (pre_gate * sig * pre_up).astype(bf16)
    own_probs = lax.dynamic_slice_in_dim(probs, zl * n, n, axis=0)[:, :1].astype(f32)
    hidden_grad = own_probs * back_hidden
    gate_pre = (hidden_grad * pre_up * sig * (1.0 + pre_gate * (1.0 - sig))).astype(bf16)
    up_pre = (hidden_grad * pre_gate * sig).astype(bf16)
    prob_part = jnp.sum(hidden.astype(f32) * back_hidden, axis=1)

    act = laid_out(zl, [gate_pre, up_pre], [ring_gather(gate_pre), ring_gather(up_pre)])
    act_mate = moved(act, "c", ring(2, 1))
    hid_rings = ring_gather(hidden)
    hid_own = laid_out(zl, [hidden], [hid_rings])
    hid_mate = moved(hid_own, "c", ring(2, 1))

    back_in = dot(act, in_own, ((1,), (1,)))
    back_in = back_in + dot(act_mate, in_other, ((1,), (1,)))
    h = n // 2
    far = back_in[2 * n : 3 * n].astype(bf16)
    from_left = moved(far[:h], "x", ring(4, 1)).astype(f32)
    from_right = moved(far[h:], "x", ring(4, -1)).astype(f32)
    one = jnp.concatenate([back_in[n : n + h] + from_left, back_in[n + h : 2 * n]], axis=0)
    three = jnp.concatenate([back_in[3 * n : 3 * n + h], back_in[3 * n + h :] + from_right], axis=0)
    summed = back_in[:n] + moved(one.astype(bf16), "x", ring(4, 1)).astype(f32)
    summed = summed + moved(three.astype(bf16), "x", ring(4, -1)).astype(f32)
    summed = summed[:h] + moved(summed[h:].astype(bf16), "zh", ring(2, 1)).astype(f32)
    summed = summed.reshape(EXPERTS, CAP, width)
    summed_rows = jnp.concatenate([summed[0]] + [moved(summed[j], "y", ring(4, -j)) for j in range(1, 4)], axis=0)

    v = prob_part.reshape(2, n // 2)
    v = v + moved(v, "c", ring(2, 1))
    v = moved(v, ("x", "zl"), [(4 * a + b, 4 * ((a + b) % 4) + b) for a in range(4) for b in range(4)])
    v = v + sum(moved(v, "zl", ring(4, j)) for j in range(1, 4))
    v = v[0] + moved(v[1], "zh", ring(2, 1))
    v = v.reshape(EXPERTS, CAP)
    summed_probs = jnp.concatenate([v[0]] + [moved(v[j], "y", ring(4, -j)) for j in range(1, 4)])

    scaled = (probs[:, :1].astype(f32) * own_grads.astype(f32)).astype(bf16)

    def canonical(own, mate):
        return [jnp.where(c == 0, own, mate), jnp.where(c == 0, mate, own)]

    pair = canonical(act, act_mate)
    gate_all = jnp.concatenate([v[:, :half] for v in pair], axis=1)
    up_all = jnp.concatenate([v[:, half:] for v in pair], axis=1)
    hidden_all = jnp.concatenate(canonical(hid_own, hid_mate), axis=1)
    gate_grad = dot(rows, gate_all, ((0,), (0,))).astype(bf16)
    up_grad = dot(rows, up_all, ((0,), (0,))).astype(bf16)
    down_grad = dot(hidden_all, scaled, ((0,), (0,))).astype(bf16)

    input_grad = lax.dot_general(
        token_pick.astype(f32),
        summed_rows,
        (((0,), (0,)), ((), ())),
        precision=precise,
        preferred_element_type=f32,
    ).astype(bf16)
    prob_grad = lax.dot_general(
        slot_pick.astype(f32),
        summed_probs,
        (((0,), (0,)), ((), ())),
        precision=precise,
        preferred_element_type=f32,
    ).reshape(-1, 2)
    return (input_grad, prob_grad, gate_grad, up_grad, down_grad)


def solution(mesh):
    names, sizes = zip(*FINE)
    fine = Mesh(mesh.devices.reshape(sizes), names)
    dp, tensor = ("y", "zh", "x"), ("zl", "c")
    return jax.shard_map(
        body,
        mesh=fine,
        in_specs=(
            P(dp, tensor),
            P(dp, tensor),
            P(dp, None),
            P(dp, None),
            P(tensor, dp),
            P(tensor, dp),
            P(dp, tensor),
        ),
        out_specs=(
            P(dp, tensor),
            P(dp, None),
            P(tensor, dp),
            P(tensor, dp),
            P(dp, tensor),
        ),
        check_vma=False,
    )
```

```python
import jax
import jax.numpy as jnp
from jax import lax
from jax.experimental import pallas as pl
from jax.experimental.pallas import tpu as pltpu
from jax.sharding import Mesh, PartitionSpec as P


EXPERTS = 4
CAP = 32
FINE = (("y", 4), ("zh", 2), ("x", 4), ("zl", 4), ("c", 2))

bf16, f32 = jnp.bfloat16, jnp.float32
precise = lax.Precision.HIGHEST


def ring(n, step):
    return [(i, (i + step) % n) for i in range(n)]


def moved(value, axis, pairs):
    return lax.ppermute(value, axis, pairs)


def dot(left, right, dims):
    return lax.dot_general(left, right, (dims, ((), ())), preferred_element_type=f32)


def slot_table(expert_ids, y):
    labels = jnp.bitwise_and(expert_ids.reshape(-1) - y, EXPERTS - 1)
    onehot = (labels[:, None] == jnp.arange(EXPERTS, dtype=jnp.int32)[None, :]).astype(jnp.int32)
    before = jnp.cumsum(onehot, axis=0) - onehot
    places = jnp.sum(before * onehot, axis=1)
    codes = labels * CAP + places
    return jnp.arange(EXPERTS * CAP, dtype=jnp.int32)[:, None] == codes[None, :]


def dispatch(block):
    got = [block[0]] + [moved(block[j], "y", ring(4, j)) for j in range(1, 4)]
    mine = jnp.concatenate(got, axis=0)
    h = mine.shape[0]
    b0 = jnp.concatenate([mine, moved(mine, "zh", ring(2, 1))], axis=0)
    b1 = moved(b0, "x", ring(4, -1))
    b3 = moved(b0, "x", ring(4, 1))
    b2a = moved(b1[:h], "x", ring(4, -1))
    b2b = moved(b3[h:], "x", ring(4, 1))
    return jnp.concatenate([b0, b1, b3, b2a, b2b], axis=0)


def ring_sum(part):
    right = left = None
    for t in range(1, 4):
        r = part(4 - t, 0) if right is None else part(4 - t, 0) + right.astype(f32)
        l = part(t, 1) if left is None else part(t, 1) + left.astype(f32)
        r, l = r.astype(bf16), l.astype(bf16)
        right = moved(r, "zl", ring(4, 1))
        left = moved(l, "zl", ring(4, -1))
        right, left = lax.optimization_barrier((right, left))
    return jnp.concatenate([part(0, 0) + right.astype(f32), part(0, 1) + left.astype(f32)], axis=0)


def laid_out(zl, owns, rings):
    n, width = owns[0].shape
    h = n // 2

    def copy(at, *refs):
        out, i = refs[-1], at[0]
        for k in range(len(owns)):
            own, r1, r2, r3, l1, l2, l3 = refs[7 * k : 7 * k + 7]

            def put(first, value):
                out[pl.ds(pl.multiple_of(first, h), h), k * width : (k + 1) * width] = value

            put(i * n, own[:h, :])
            put(i * n + h, own[h:, :])
            for t, (r, l) in enumerate(((r1, l1), (r2, l2), (r3, l3)), start=1):
                put(((i + 4 - t) & 3) * n, r[...])
                put(((i + t) & 3) * n + h, l[...])

    whole = pl.BlockSpec(memory_space=pltpu.VMEM)
    pieces = sum([[own] + rights + lefts for own, (rights, lefts) in zip(owns, rings)], [])
    return pl.pallas_call(
        copy,
        out_shape=jax.ShapeDtypeStruct((4 * n, width * len(owns)), owns[0].dtype),
        in_specs=[pl.BlockSpec(memory_space=pltpu.SMEM)] + [whole] * len(pieces),
        out_specs=whole,
    )(zl.reshape(1), *pieces)


def ring_gather(own):
    h = own.shape[0] // 2
    rights, lefts = [own[:h]], [own[h:]]
    for _ in range(1, 4):
        rights.append(moved(rights[-1], "zl", ring(4, 1)))
        lefts.append(moved(lefts[-1], "zl", ring(4, -1)))
    return rights[1:], lefts[1:]


def body(tokens, out_grad, expert_ids, gate_prob, gate_weight, up_weight, down_weight):
    y, zl, c = lax.axis_index("y"), lax.axis_index("zl"), lax.axis_index("c")
    width = tokens.shape[1]
    hid = gate_weight.shape[1]
    half = hid // 2

    selector = slot_table(expert_ids, y)
    token_pick = jnp.any(selector.reshape(EXPERTS * CAP, -1, 2), axis=2).astype(bf16)
    slot_pick = selector.astype(bf16)
    send_rows = dot(token_pick, tokens, ((1,), (0,))).astype(bf16)
    send_grads = dot(token_pick, out_grad, ((1,), (0,))).astype(bf16)
    send_probs = dot(slot_pick, gate_prob.reshape(-1, 1), ((1,), (0,))).astype(bf16)
    send_grads = jnp.concatenate([send_grads, jnp.broadcast_to(send_probs, (EXPERTS * CAP, 128))], axis=1)

    def halves(weight, axis):
        return lax.optimization_barrier(
            [lax.dynamic_slice_in_dim(weight, s * half, half, axis) for s in (c, 1 - c)]
        )

    sides = [halves(gate_weight, 1), halves(up_weight, 1)]
    in_own, in_other = (jnp.concatenate([sides[0][s], sides[1][s]], axis=1) for s in range(2))
    out_own, out_other = halves(down_weight, 0)
    gate_mate = moved(sides[0][1], "c", ring(2, 1))
    up_mate = moved(sides[1][1], "c", ring(2, 1))
    out_mate = moved(out_other, "c", ring(2, 1))

    rows = dispatch(send_rows.reshape(EXPERTS, CAP, width))
    grads = dispatch(send_grads.reshape(EXPERTS, CAP, width + 128))
    n = rows.shape[0] // 4
    rows_mate = moved(rows, "c", ring(2, 1))
    grads_mate = moved(grads, "c", ring(2, 1))
    probs = grads[:, width:]
    own_grads = grads[:, :width]

    gate_sum = dot(rows_mate, gate_mate, ((1,), (0,)))
    gate_sum = gate_sum + dot(rows, sides[0][0], ((1,), (0,)))
    up_sum = dot(rows_mate, up_mate, ((1,), (0,)))
    up_sum = up_sum + dot(rows, sides[1][0], ((1,), (0,)))
    bh = dot(grads_mate[:, :width], out_mate, ((1,), (1,)))
    bh = bh + dot(own_grads, out_own, ((1,), (1,)))

    def part_of(value):
        def part(j, s):
            at = jnp.bitwise_and(zl + j, 3) * n + s * (n // 2)
            return lax.dynamic_slice_in_dim(value, at, n // 2, axis=0)

        return part

    pre_gate = ring_sum(part_of(gate_sum))
    pre_up = ring_sum(part_of(up_sum))
    back_hidden = ring_sum(part_of(bh))
    sig = jax.nn.sigmoid(pre_gate)
    hidden = (pre_gate * sig * pre_up).astype(bf16)
    own_probs = lax.dynamic_slice_in_dim(probs, zl * n, n, axis=0)[:, :1].astype(f32)
    hidden_grad = own_probs * back_hidden
    gate_pre = (hidden_grad * pre_up * sig * (1.0 + pre_gate * (1.0 - sig))).astype(bf16)
    up_pre = (hidden_grad * pre_gate * sig).astype(bf16)
    prob_part = jnp.sum(hidden.astype(f32) * back_hidden, axis=1)

    act = laid_out(zl, [gate_pre, up_pre], [ring_gather(gate_pre), ring_gather(up_pre)])
    act_mate = moved(act, "c", ring(2, 1))
    hid_rings = ring_gather(hidden)
    hid_own = laid_out(zl, [hidden], [hid_rings])
    hid_mate = moved(hid_own, "c", ring(2, 1))

    back_in = dot(act, in_own, ((1,), (1,)))
    back_in = back_in + dot(act_mate, in_other, ((1,), (1,)))
    h = n // 2
    far = back_in[3 * n :].astype(bf16)
    from_left = moved(far[:h], "x", ring(4, 1)).astype(f32)
    from_right = moved(far[h:], "x", ring(4, -1)).astype(f32)
    one = jnp.concatenate([back_in[n : n + h] + from_left, back_in[n + h : 2 * n]], axis=0)
    three = jnp.concatenate([back_in[2 * n : 2 * n + h], back_in[2 * n + h : 3 * n] + from_right], axis=0)
    summed = back_in[:n] + moved(one.astype(bf16), "x", ring(4, 1)).astype(f32)
    summed = summed + moved(three.astype(bf16), "x", ring(4, -1)).astype(f32)
    summed = summed[:h] + moved(summed[h:].astype(bf16), "zh", ring(2, 1)).astype(f32)
    summed = summed.reshape(EXPERTS, CAP, width)
    summed_rows = jnp.concatenate([summed[0]] + [moved(summed[j], "y", ring(4, -j)) for j in range(1, 4)], axis=0)

    v = prob_part.reshape(2, n // 2)
    v = v + moved(v, "c", ring(2, 1))
    v = moved(v, ("x", "zl"), [(4 * a + b, 4 * ((a + f) % 4) + b) for a in range(4) for b, f in enumerate((0, 1, 3, 2))])
    v = v + moved(v, "zl", ring(4, 1))
    v = v + moved(v, "zl", ring(4, 2))
    v = v[0] + moved(v[1], "zh", ring(2, 1))
    v = v.reshape(EXPERTS, CAP)
    summed_probs = jnp.concatenate([v[0]] + [moved(v[j], "y", ring(4, -j)) for j in range(1, 4)])

    scaled = (probs[:, :1].astype(f32) * own_grads.astype(f32)).astype(bf16)

    def canonical(own, mate):
        return [jnp.where(c == 0, own, mate), jnp.where(c == 0, mate, own)]

    pair = canonical(act, act_mate)
    gate_all = jnp.concatenate([v[:, :half] for v in pair], axis=1)
    up_all = jnp.concatenate([v[:, half:] for v in pair], axis=1)
    hidden_all = jnp.concatenate(canonical(hid_own, hid_mate), axis=1)
    gate_grad = dot(rows, gate_all, ((0,), (0,))).astype(bf16)
    up_grad = dot(rows, up_all, ((0,), (0,))).astype(bf16)
    down_grad = dot(hidden_all, scaled, ((0,), (0,))).astype(bf16)

    input_grad = lax.dot_general(
        token_pick.astype(f32),
        summed_rows,
        (((0,), (0,)), ((), ())),
        precision=precise,
        preferred_element_type=f32,
    ).astype(bf16)
    prob_grad = lax.dot_general(
        slot_pick.astype(f32),
        summed_probs,
        (((0,), (0,)), ((), ())),
        precision=precise,
        preferred_element_type=f32,
    ).reshape(-1, 2)
    return (input_grad, prob_grad, gate_grad, up_grad, down_grad)


def solution(mesh):
    names, sizes = zip(*FINE)
    fine = Mesh(mesh.devices.reshape(sizes), names)
    dp, tensor = ("y", "zh", "x"), ("zl", "c")
    return jax.shard_map(
        body,
        mesh=fine,
        in_specs=(
            P(dp, tensor),
            P(dp, tensor),
            P(dp, None),
            P(dp, None),
            P(tensor, dp),
            P(tensor, dp),
            P(dp, tensor),
        ),
        out_specs=(
            P(dp, tensor),
            P(dp, None),
            P(tensor, dp),
            P(tensor, dp),
            P(dp, tensor),
        ),
        check_vma=False,
    )
```
